256 devices in a mesh: dp: 2 (over x_lo), fsdp: 16 (over x_hi, y, core), tensor: 8 (over z).
Axes of the slice: x: 4 (x_hi: 2, x_lo: 2; x = x_hi * 2 + x_lo), y: 4, z: 8, core: 2. Of those that a mesh axis runs over, the one named last changes fastest.
Arguments:
- hidden: bfloat16 [16384, 2048], P(('dp', 'fsdp'), 'tensor'), may hold values from -8 to 8
- norm_gain: bfloat16 [2048], P('tensor'), may hold values from 0.099609375 to 1.8984375
- head_weight: bfloat16 [2048, 32128], P('fsdp', 'tensor'), may hold values from -1 to 1
- token_ids: int32 [32, 512], P(('dp', 'fsdp')), may hold values from 0 to 32127
- lengths: int32 [32], P(('dp', 'fsdp')), may hold values from 128 to 512
- old_logp: float32 [32, 512], P(('dp', 'fsdp')), may hold values from -12.5 to -9.5
- advantages: float32 [32, 512], P(('dp', 'fsdp')), may hold values from -4 to 4
- rollout_logp: float32 [32, 512], P(('dp', 'fsdp'), 'tensor'), may hold values from -16 to -1
- rollout_row: int32 [32], P(('dp', 'fsdp')), may hold values from 0 to 31, each once
Outputs:
- new_logp: float32 [32, 512], P(('dp', 'fsdp'))
- token_loss: float32 [32, 512], P(('dp', 'fsdp'))
- summary: float32 [3], replicated
The draws below stay inside these ranges and needn't reach their ends.
Inputs may be any that keep to these rules, and one draw needn't show every extreme that they name: `rollout_row`: every row 0 to 31 is named once.
All inputs are finite; a program needn't handle non-finite values.
Results may differ from the reference program's by a relative error of at most 0.0005.
The reference program's roundings to bfloat16 on the way (of `normed`) count: a program that leaves them out, or rounds other values in their place, can miss the bound.
Values may be sent and summed in bfloat16 or wider, within the bound.
No kernel may reach another device: no remote copies, remote signals or barrier semaphores. Data moves between devices by JAX's collectives and lax.ppermute only.
A program may use at most 128 MiB of HBM per device.

```python
import math
import jax
import jax.numpy as jnp
import numpy as np
from jax import lax

D = 2048
VOCAB = 32128
LEN = 512
RESP = 32
TOKENS = 16384


def draw_hidden(key, part):
    samples = jax.random.normal(jax.random.fold_in(key, 21), (TOKENS, D), jnp.float32)
    return jnp.clip(samples, -8.0, 8.0).astype(jnp.bfloat16)


def draw_head_weight(key, part):
    weights = jax.random.normal(jax.random.fold_in(key, 31), (D, VOCAB), jnp.float32) / math.sqrt(D)
    return jnp.clip(weights, -1.0, 1.0).astype(jnp.bfloat16)


def draw_lengths(key, part):
    row_index = jnp.arange(RESP, dtype=jnp.int32)
    shortest = LEN // 4
    rising = shortest + row_index * (LEN - shortest) // max(RESP - 1, 1)
    jitter = jax.random.randint(jax.random.fold_in(key, 41), (RESP,), 0, LEN // 8 + 1)
    values = jnp.clip(rising - jitter, shortest, LEN)
    values = jnp.where(row_index == RESP - 1, LEN, values)
    values = jnp.where(row_index == 0, shortest, values)
    return values.astype(jnp.int32)


def draw_rollout_logp(key, part):
    center = -math.log(VOCAB)
    row_offset = jax.random.uniform(jax.random.fold_in(key, 51), (RESP, 1), jnp.float32, -2.0, 2.0)
    token_jitter = jax.random.uniform(jax.random.fold_in(key, 52), (RESP, LEN), jnp.float32, -1.0, 1.0)
    return jnp.clip(center + row_offset + token_jitter, -16.0, -1.0)


def with_ends(array, rng, smallest, largest):
    longest = array.shape.index(max(array.shape))
    spots = []
    for shift in (0, 1):
        where = [jax.random.randint(jax.random.fold_in(rng, axis), (), 0, length) for axis, length in enumerate(array.shape)]
        where[longest] = (where[longest] + shift) % array.shape[longest]
        spots.append(tuple(where))
    return array.at[spots[0]].set(smallest).at[spots[1]].set(largest)


def block_levels(key, dims, cuts, low, high):
    loudness, own = 1.0, jax.random.fold_in(key, 6)
    for dim, parts in cuts:
        draws = jnp.exp(jax.random.uniform(jax.random.fold_in(own, dim), (parts,), jnp.float32, low / len(cuts), high / len(cuts)))
        loudness = loudness * jnp.repeat(draws, dims[dim] // parts).reshape([-1 if axis == dim else 1 for axis in range(len(dims))])
    return loudness


def cumulative_ranks(amount, slope):
    portions = [(1 << 20) // math.isqrt(rank ** slope) + 1 for rank in range(1, amount + 1)]
    deviation = 1 + sum(portions) // (1 << 30)
    return np.cumsum(np.array([max(1, weight // deviation) for weight in portions]))


def ranked_ids(stream_key, extent, amount, skew):
    listing = cumulative_ranks(amount, skew)
    lot = jax.random.randint(jax.random.fold_in(stream_key, 1), extent, 0, int(listing[amount - 1]))
    standing = jnp.searchsorted(jnp.asarray(listing, jnp.int32), lot, side="right")
    return jax.random.permutation(jax.random.fold_in(stream_key, 2), amount)[standing].astype(jnp.int32)


def noise(own_key, extent, deviation, most, cuts=(), kind=jnp.bfloat16):
    drawn = jax.random.normal(own_key, extent, jnp.float32) * deviation
    if len(cuts) > 0:
        drawn = block_levels(own_key, extent, cuts, -0.22, 0.18) * drawn
    return jnp.clip(drawn, min=-most, max=most).astype(kind)


def setup_inputs(seed: int = 0) -> dict:
    splits = jax.random.split(jax.random.key(seed), 10)
    hidden = draw_hidden(jax.random.fold_in(splits[9], 71), 0)
    norm_gain = jnp.clip(1.0 + 0.18 * jax.random.normal(splits[1], (D,), jnp.float32), 0.099609375, 1.8984375).astype(jnp.bfloat16)
    head_weight = draw_head_weight(jax.random.fold_in(splits[9], 71), 0)
    token_ids = with_ends(ranked_ids(splits[3], (RESP, LEN), VOCAB, 2), jax.random.fold_in(splits[3], 3), 0, VOCAB - 1).astype(jnp.int32)
    lengths = draw_lengths(jax.random.fold_in(splits[9], 71), 0)
    old_logp = jnp.clip(-12.5 + 3.0 * jax.random.uniform(splits[5], (RESP, LEN), jnp.float32) ** block_levels(splits[5], (RESP, LEN), ((0, 32),), -0.2, 0.2), -12.5, -9.5)
    advantages = noise(splits[6], (RESP, LEN), 1.0, 4.0, ((0, 32),), jnp.float32)
    rollout_logp = draw_rollout_logp(jax.random.fold_in(splits[9], 71), 0)
    rollout_row = jax.random.permutation(splits[8], RESP).astype(jnp.int32)
    return {"hidden": hidden, "norm_gain": norm_gain, "head_weight": head_weight, "token_ids": token_ids, "lengths": lengths, "old_logp": old_logp, "advantages": advantages, "rollout_logp": rollout_logp, "rollout_row": rollout_row}


clip_eps = 0.2
kl_coef = 0.2
log_limit = 10.0
norm_eps = 1e-06

def token_terms(new_logp, old_logp, advantages, ref_logp, live_mask, prob_square):
    shift = new_logp - old_logp
    prob_ratio = jnp.exp(jnp.clip(shift, -log_limit, log_limit))
    clipped = jnp.clip(prob_ratio, 1.0 - clip_eps, 1.0 + clip_eps)
    plain_term = prob_ratio * advantages
    bounded_term = clipped * advantages
    surrogate = jnp.minimum(plain_term, bounded_term)
    ref_gap = ref_logp - new_logp
    gap_clip = jnp.clip(ref_gap, -log_limit, log_limit)
    kl_term = jnp.exp(gap_clip) - gap_clip - 1.0
    token_loss = live_mask * (kl_coef * kl_term - surrogate)
    inside_gap = (jnp.abs(ref_gap) < log_limit).astype(jnp.float32)
    inside_ratio = (jnp.abs(shift) < log_limit).astype(jnp.float32)
    active_term = (plain_term <= bounded_term).astype(jnp.float32)
    grad_coef = live_mask * (kl_coef * (1.0 - jnp.exp(gap_clip)) * inside_gap - advantages * prob_ratio * active_term * inside_ratio)
    grad_square = grad_coef * grad_coef * (prob_square - 2.0 * jnp.exp(new_logp) + 1.0)
    return (token_loss, live_mask * kl_term, grad_square)

def reference(hidden, norm_gain, head_weight, token_ids, lengths, old_logp, advantages, rollout_logp, rollout_row):
    values = hidden.astype(jnp.float32)
    inv_rms = lax.rsqrt(lax.optimization_barrier(jnp.mean(values * values, axis=1, keepdims=True)) + norm_eps)
    normed = (values * inv_rms * norm_gain.astype(jnp.float32)[None, :]).astype(jnp.bfloat16)
    blocks = normed.reshape(token_ids.shape[0], token_ids.shape[1], normed.shape[1])

    def per_response(block):
        block_rows, block_ids = block
        logits = jnp.dot(block_rows, head_weight, preferred_element_type=jnp.float32)
        row_max = lax.optimization_barrier(jnp.max(logits, axis=1))
        shifted = jnp.exp(logits - row_max[:, None])
        exp_sum = lax.optimization_barrier(jnp.sum(shifted, axis=1))
        exp_square = lax.optimization_barrier(jnp.sum(shifted * shifted, axis=1))
        picked = jnp.take_along_axis(logits, block_ids[:, None].astype(jnp.int32), axis=1)[:, 0]
        return (picked - row_max - jnp.log(exp_sum), exp_square / (exp_sum * exp_sum))
    new_logp, prob_square = lax.map(per_response, (blocks, token_ids))
    ref_logp = jnp.take(rollout_logp, rollout_row.astype(jnp.int32), axis=0)
    positions = lax.broadcasted_iota(jnp.int32, token_ids.shape, 1)
    live_mask = (positions < lengths[:, None]).astype(jnp.float32)
    token_loss, kl_part, grad_part = token_terms(new_logp, old_logp, advantages, ref_logp, live_mask, prob_square)
    live_count = jnp.sum(live_mask)
    summary = jnp.stack([jnp.sum(token_loss) / live_count, jnp.sum(kl_part) / live_count, jnp.sqrt(jnp.sum(grad_part) / live_count)])
    return (new_logp, token_loss, summary)
```

```python
import jax
import jax.numpy as jnp
from jax import lax
from jax.experimental import pallas as pl
from jax.experimental.pallas import tpu as pltpu
from jax.sharding import Mesh, PartitionSpec as P


clip_eps = 0.2
kl_coef = 0.2
log_limit = 10.0
norm_eps = 1e-06

HALF = 2048
ROWS = 128
FEAT = 256
TOK = 512
BLOCK = 512


def shift(n, k):
    return [(i, (i + k) % n) for i in range(n)]


def x_position(x):
    return (x % 2) * 2 + x // 2


X_NEAR = [(x_position(a), x_position(b)) for a, b in ((1, 2), (2, 1), (3, 0), (0, 3))]


def head_kernel(where_ref, *refs):
    toks = refs[:18]
    heads = refs[18:38]
    ids_ref, out_ref, w_buf, t_buf, lhs, gain, inv, logits, sem_t, sem_w = refs[38:]
    tensor, xh, y, core, dp = [where_ref[0, i] for i in range(5)]
    valid = where_ref[0, 5]

    copies = []
    slot_of = {0: 0, 1: -1, 2: 1, 3: -2, 4: 2, 5: -3, 6: 3, 7: 4}
    for side in range(2):
        for k in range(9):
            ref = toks[side * 9 + k]
            if k < 7:
                dst = t_buf.at[side, k, pl.ds(0, ref.shape[0])]
            elif k == 7:
                dst = t_buf.at[side, 7, pl.ds(0, 256)]
            else:
                dst = t_buf.at[side, 7, pl.ds(256, ref.shape[0])]
            c = pltpu.make_async_copy(ref, dst, sem_t)
            c.start()
            copies.append(c)
    wcopies = []
    row = 0
    for ref in heads:
        c = pltpu.make_async_copy(ref, w_buf.at[pl.ds(row, ref.shape[0])], sem_w)
        c.start()
        wcopies.append(c)
        row += ref.shape[0]
    for c in copies:
        c.wait()

    def place(k):
        z = lax.rem(tensor + slot_of[k] + 8, 8)
        zh, zy = lax.div(z, 4), lax.rem(z, 4)
        step = lax.rem(zy - y + 4, 4)
        order = jnp.where(step == 0, 0, jnp.where(step == 3, 1, jnp.where(step == 1, 2, 3)))
        return jnp.where(zh == xh, 0, 4) + order

    for side in range(2):
        def squares(i, _):
            rows = pl.ds(i * 64, 64)
            total = jnp.zeros((64, 128), jnp.float32)
            for k in range(8):
                v = t_buf[side, k, rows, :].astype(jnp.float32)
                v = v * v
                total = total + v[:, :128] + v[:, 128:]
            mean = jnp.sum(total, axis=1, keepdims=True) * (1.0 / 2048)
            inv[pl.ds(side * TOK + i * 64, 64), :] = jnp.broadcast_to(lax.rsqrt(mean + norm_eps), (64, 128))
            return 0
        lax.fori_loop(0, 8, squares, 0)
    for k in range(8):
        at = place(k)
        g = t_buf[0, k, 512:513, :].astype(jnp.float32)
        for side in range(2):
            def normed(i, _):
                rows = pl.ds(i * 64, 64)
                out = pl.ds(side * TOK + i * 64, 64)
                v = t_buf[side, k, rows, :].astype(jnp.float32)
                scale = inv[out, :]
                for h in range(2):
                    part = v[:, h * 128 : h * 128 + 128] * scale * g[:, h * 128 : h * 128 + 128]
                    lane = pl.multiple_of(at * 256 + (core ^ h) * 128, 128)
                    lhs[out, pl.ds(lane, 128)] = part.astype(jnp.bfloat16)
                return 0
            lax.fori_loop(0, 8, normed, 0)
    for c in wcopies:
        c.wait()

    for m in range(2 * TOK // BLOCK):
        logits[...] = jnp.dot(lhs[m * BLOCK : (m + 1) * BLOCK, :], w_buf[...], preferred_element_type=jnp.float32)

        def stats(i, _):
            rows = pl.ds(i * 64, 64)
            lanes = lax.broadcasted_iota(jnp.int32, (64, 128), 1)
            top = None
            for j in range(HALF // 128):
                x = logits[rows, j * 128 : (j + 1) * 128]
                if (j + 1) * 128 > 1968 - 127:
                    x = jnp.where(lanes < valid - j * 128, x, -jnp.inf)
                top = x if top is None else jnp.maximum(top, x)
            top = jnp.max(top, axis=1, keepdims=True)
            ids = ids_ref[pl.ds(m * BLOCK + i * 64, 64), :]
            s = jnp.zeros((64, 128), jnp.float32)
            q = jnp.zeros((64, 128), jnp.float32)
            p = jnp.zeros((64, 128), jnp.float32)
            for j in range(HALF // 128):
                x = logits[rows, j * 128 : (j + 1) * 128]
                e = jnp.exp(x - top)
                if (j + 1) * 128 > 1968 - 127:
                    ok = lanes < valid - j * 128
                    e = jnp.where(ok, e, 0.0)
                s = s + e
                q = q + e * e
                p = p + jnp.where(lanes == ids - j * 128, x, 0.0)
            s = jnp.sum(s, axis=1, keepdims=True)
            q = jnp.sum(q, axis=1, keepdims=True)
            p = jnp.sum(p, axis=1, keepdims=True)
            tile = jnp.where(lanes == 0, top, jnp.where(lanes == 1, s, jnp.where(lanes == 2, q, p)))
            inv[pl.ds(m * BLOCK + i * 64, 64), :] = tile
            return 0
        lax.fori_loop(0, BLOCK // 64, stats, 0)
    for i in range(2 * TOK // 128):
        out_ref[:, i * 128 : (i + 1) * 128] = jnp.transpose(inv[i * 128 : (i + 1) * 128, :])[:8, :]


def head_stats(where, toks, heads, ids):
    any_spec = pl.BlockSpec(memory_space=pl.ANY)
    n = len(toks) + len(heads)
    return pl.pallas_call(
        head_kernel,
        out_shape=jax.ShapeDtypeStruct((8, 2 * TOK), jnp.float32),
        in_specs=[pl.BlockSpec(memory_space=pltpu.SMEM)] + [any_spec] * n + [pl.BlockSpec(memory_space=pltpu.VMEM)],
        out_specs=pl.BlockSpec(memory_space=pltpu.VMEM),
        scratch_shapes=[
            pltpu.VMEM((2048, HALF), jnp.bfloat16),
            pltpu.VMEM((2, 8, TOK + 16, FEAT), jnp.bfloat16),
            pltpu.VMEM((2 * TOK, 2048), jnp.bfloat16),
            pltpu.VMEM((8, FEAT), jnp.float32),
            pltpu.VMEM((2 * TOK, 128), jnp.float32),
            pltpu.VMEM((BLOCK, HALF), jnp.float32),
            pltpu.SemaphoreType.DMA,
            pltpu.SemaphoreType.DMA,
        ],
        compiler_params=pltpu.CompilerParams(vmem_limit_bytes=48 * 1024 * 1024),
        name="head_stats",
    )(where, *toks, *heads, ids)


def token_terms(new_logp, old_logp, advantages, ref_logp, live_mask, prob_square):
    diff = new_logp - old_logp
    prob_ratio = jnp.exp(jnp.clip(diff, -log_limit, log_limit))
    clipped = jnp.clip(prob_ratio, 1.0 - clip_eps, 1.0 + clip_eps)
    plain_term = prob_ratio * advantages
    bounded_term = clipped * advantages
    surrogate = jnp.minimum(plain_term, bounded_term)
    ref_gap = ref_logp - new_logp
    gap_clip = jnp.clip(ref_gap, -log_limit, log_limit)
    kl_term = jnp.exp(gap_clip) - gap_clip - 1.0
    token_loss = live_mask * (kl_coef * kl_term - surrogate)
    inside_gap = (jnp.abs(ref_gap) < log_limit).astype(jnp.float32)
    inside_ratio = (jnp.abs(diff) < log_limit).astype(jnp.float32)
    active_term = (plain_term <= bounded_term).astype(jnp.float32)
    grad_coef = live_mask * (
        kl_coef * (1.0 - jnp.exp(gap_clip)) * inside_gap
        - advantages * prob_ratio * active_term * inside_ratio
    )
    grad_square = grad_coef * grad_coef * (prob_square - 2.0 * jnp.exp(new_logp) + 1.0)
    return (token_loss, live_mask * kl_term, grad_square)


def token_ring(own):
    back, ahead = [own], [own]
    for _ in range(3):
        back.append(lax.ppermute(back[-1], "tensor", shift(8, 1)))
        ahead.append(lax.ppermute(ahead[-1], "tensor", shift(8, -1)))
    far_a = lax.ppermute(back[3][:256], "tensor", shift(8, 1))
    far_b = lax.ppermute(ahead[3][256:], "tensor", shift(8, -1))
    return [own, back[1], ahead[1], back[2], ahead[2], back[3], ahead[3], far_a, far_b]


def head_ring(own):
    back = lax.ppermute(own, "y", shift(4, 1))
    ahead = lax.ppermute(own, "y", shift(4, -1))
    far_a = lax.ppermute(back[: ROWS // 2], "y", shift(4, 1))
    far_b = lax.ppermute(ahead[ROWS // 2 :], "y", shift(4, -1))
    pieces = [[own], [back], [ahead], [far_a, far_b]]
    out = []
    for piece in pieces:
        out += piece + [lax.ppermute(p, "core", shift(2, 1)) for p in piece]
    return out


def shards(
    hidden,
    norm_gain,
    head_weight,
    token_ids,
    lengths,
    old_logp,
    advantages,
    rollout_logp,
    rollout_row,
):
    dp, xh, y, core, tensor = [lax.axis_index(a) for a in ("dp", "xh", "y", "core", "tensor")]
    cols = head_weight.shape[1]
    low = head_weight[:, :HALF]
    high = jnp.pad(head_weight[:, HALF:], ((0, 0), (0, 2 * HALF - cols)))
    mine = jnp.where(dp == 0, low, high)
    other = jnp.where(dp == 0, high, low)

    stream = jnp.concatenate([hidden, jnp.broadcast_to(norm_gain[None, :], (16, FEAT))])
    partner = lax.ppermute(hidden, "dp", shift(2, 1))
    near = lax.ppermute(other, ("dp", "xh"), X_NEAR)
    heads = head_ring(mine) + head_ring(near)
    toks = token_ring(stream) + token_ring(partner)

    partner_ids = lax.ppermute(token_ids, "dp", shift(2, 1))
    local = jnp.concatenate([token_ids, partner_ids], axis=1).reshape(-1) - (tensor * cols + dp * HALF)
    in_half = (local >= 0) & (local < jnp.where(dp == 0, HALF, cols - HALF))
    local = jnp.where(in_half, local, -1)
    ids = jnp.broadcast_to(local[:, None], (2 * TOK, 128))
    valid = jnp.where(dp == 0, HALF, cols - HALF)
    where = jnp.stack([tensor, xh, y, core, dp, valid, valid, valid]).astype(jnp.int32)[None, :]

    refs = jnp.broadcast_to(rollout_logp, (32, 1, 64))
    refs = lax.all_to_all(refs, ("dp", "xh", "y", "core"), 0, 0, tiled=True)
    own_ref = lax.dynamic_index_in_dim(refs[:, 0], rollout_row[0], 0, keepdims=False)

    stats = head_stats(where, toks, heads, ids)
    stats = stats[:4]
    mine_s, part_s = stats[:, :TOK].reshape(-1), stats[:, TOK:].reshape(-1)
    by_dp = jnp.stack([jnp.where(dp == 0, mine_s, part_s), jnp.where(dp == 0, part_s, mine_s)])
    by_dp = jnp.concatenate([by_dp, jnp.broadcast_to(own_ref[None], (2, 64))], axis=1)
    send = jnp.broadcast_to(by_dp[:, None], (2, 8, 4 * TOK + 64)).reshape(16, 1, 4 * TOK + 64)
    got = lax.all_to_all(send, ("dp", "tensor"), 0, 0, tiled=True).reshape(16, 4 * TOK + 64)
    tops, sums, squares, picks = [got[:, i * TOK : (i + 1) * TOK] for i in range(4)]
    ref_logp = jnp.where(dp == 0, got[:8, 4 * TOK :], got[8:, 4 * TOK :]).reshape(1, TOK)
    row_max = jnp.max(tops, axis=0)
    scale = jnp.exp(tops - row_max[None])
    exp_sum = jnp.sum(sums * scale, axis=0)
    exp_square = jnp.sum(squares * scale * scale, axis=0)
    picked = jnp.sum(picks, axis=0)
    new_logp = (picked - row_max - jnp.log(exp_sum)).reshape(token_ids.shape)
    prob_square = (exp_square / (exp_sum * exp_sum)).reshape(token_ids.shape)
    positions = lax.broadcasted_iota(jnp.int32, token_ids.shape, 1)
    live_mask = (positions < lengths[:, None]).astype(jnp.float32)
    token_loss, kl_part, grad_part = token_terms(
        new_logp, old_logp, advantages, ref_logp, live_mask, prob_square
    )
    parts = jnp.stack([jnp.sum(live_mask), jnp.sum(token_loss), jnp.sum(kl_part), jnp.sum(grad_part)])
    parts = jnp.broadcast_to(parts[None, None], (32, 1, 4))
    totals = jnp.sum(lax.all_to_all(parts, ("dp", "xh", "y", "core"), 0, 0, tiled=True), axis=(0, 1))
    summary = jnp.stack([totals[1] / totals[0], totals[2] / totals[0], jnp.sqrt(totals[3] / totals[0])])
    return (new_logp, token_loss, summary)


def solution(mesh):
    fine = Mesh(mesh.devices.reshape(2, 2, 4, 2, 8), ("dp", "xh", "y", "core", "tensor"))
    rows = ("dp", "xh", "y", "core")
    in_specs = (
        P(rows, "tensor"),
        P("tensor"),
        P(("xh", "y", "core"), "tensor"),
        P(rows, None),
        P(rows),
        P(rows, None),
        P(rows, None),
        P(rows, "tensor"),
        P(rows),
    )
    out_specs = (P(rows, None), P(rows, None), P())
    return jax.shard_map(shards, mesh=fine, in_specs=in_specs, out_specs=out_specs, check_vma=False)
```

```python
import functools

import jax
import jax.numpy as jnp
from jax import lax
from jax.experimental import pallas as pl
from jax.experimental.pallas import tpu as pltpu
from jax.sharding import Mesh, PartitionSpec as P


clip_eps = 0.2
kl_coef = 0.2
log_limit = 10.0
norm_eps = 1e-06

HALF = 2048
ROWS = 128
FEAT = 256
TOK = 512
PART = TOK + 16
COLS = 256


def shift(n, k):
    return [(i, (i + k) % n) for i in range(n)]


def x_position(x):
    return (x % 2) * 2 + x // 2


X_NEAR = [(x_position(a), x_position(b)) for a, b in ((1, 2), (2, 1), (3, 0), (0, 3))]


def split_kernel(where_ref, head_ref, mine_ref, other_ref):
    cols = head_ref.shape[1]

    def place(low_ref, high_ref):
        low_ref[...] = head_ref[:, :HALF]
        high_ref[:, : cols - HALF] = head_ref[:, HALF:]
        high_ref[:, cols - HALF :] = jnp.zeros((ROWS, 2 * HALF - cols), jnp.bfloat16)

    @pl.when(where_ref[0, 4] == 0)
    def _():
        place(mine_ref, other_ref)

    @pl.when(where_ref[0, 4] != 0)
    def _():
        place(other_ref, mine_ref)


def split_head(where, head):
    half = jax.ShapeDtypeStruct((ROWS, HALF), jnp.bfloat16)
    return pl.pallas_call(
        split_kernel,
        out_shape=(half, half),
        in_specs=[pl.BlockSpec(memory_space=pltpu.SMEM), pl.BlockSpec(memory_space=pltpu.VMEM)],
        out_specs=[pl.BlockSpec(memory_space=pltpu.VMEM)] * 2,
        name="split_head",
    )(where, head)


def head_kernel(last, far_core, *refs):
    where_ref = refs[0]
    toks = refs[1:10]
    heads = refs[10:20]
    ids_ref = refs[20]
    n = 21
    if last:
        first_ref, ref_ref = refs[n : n + 2]
        n += 2
    out_ref, w_buf, t_buf, lhs, tops, sums, squares, picks, even, odd, sem_t, sem_w = refs[n:]
    tensor, xh, y, core, dp, valid = [where_ref[0, i] for i in range(6)]

    def copy(src, dst, sem):
        c = pltpu.make_async_copy(src, dst, sem)
        c.start()
        return c

    first = pl.ds(0, PART)
    second = pl.ds(PART, PART)
    t_copies = [copy(toks[0], t_buf.at[0], sem_t)]
    for k in range(3):
        t_copies.append(copy(toks[1 + 2 * k].at[first], t_buf.at[1 + 2 * k], sem_t))
        t_copies.append(copy(toks[2 + 2 * k].at[second], t_buf.at[2 + 2 * k], sem_t))

    @pl.when(core == far_core)
    def _():
        pltpu.make_async_copy(toks[7].at[first], t_buf.at[7], sem_t).start()

    @pl.when(core != far_core)
    def _():
        pltpu.make_async_copy(toks[8].at[second], t_buf.at[7], sem_t).start()

    w_copies = []
    rows = [pl.ds(i * ROWS, ROWS) for i in range(16)]
    for s in range(2):
        own, near, near_passed, far, far_passed = heads[5 * s : 5 * s + 5]
        at = 8 * s
        w_copies.append(copy(own, w_buf.at[pl.ds(at * ROWS, 2 * ROWS)], sem_w))
        w_copies.append(copy(near, w_buf.at[pl.ds((at + 2) * ROWS, 2 * ROWS)], sem_w))
        for h in range(2):
            w_copies.append(copy(near_passed.at[rows[h]], w_buf.at[rows[at + 4 + 1 - h]], sem_w))

        @pl.when(core == s)
        def _():
            for h in range(2):
                pltpu.make_async_copy(far.at[rows[h]], w_buf.at[rows[at + 6 + h]], sem_w).start()

        @pl.when(core != s)
        def _():
            for h in range(2):
                pltpu.make_async_copy(far_passed.at[rows[h]], w_buf.at[rows[at + 7 - h]], sem_w).start()

        for h in range(2):
            w_copies.append(pltpu.make_async_copy(far.at[rows[h]], w_buf.at[rows[at + 6 + h]], sem_w))
    for c in t_copies:
        c.wait()
    pltpu.make_async_copy(toks[7].at[first], t_buf.at[7], sem_t).wait()

    way = 2 * core - 1

    def place(k):
        if k == 0:
            offset = 0
        elif k == 7:
            offset = 4
        else:
            step = (k + 1) // 2
            offset = way * step if k % 2 == 1 else -way * step
        z = lax.rem(tensor + offset + 8, 8)
        zh, zy = lax.div(z, 4), lax.rem(z, 4)
        step = lax.rem(way * (zy - y) + 4, 4)
        order = jnp.where(step == 0, 0, jnp.where(step == 1, 1, jnp.where(step == 3, 2, 3)))
        return jnp.where(zh == xh, 0, 4) + order

    def square(i, _):
        at = pl.ds(i * 64, 64)
        total = jnp.zeros((64, 128), jnp.float32)
        for k in range(8):
            v = t_buf[k, at, :].astype(jnp.float32)
            v = v * v
            total = total + v[:, :128] + v[:, 128:]
        mean = jnp.sum(total, axis=1, keepdims=True) * (1.0 / 2048)
        tops[at, :] = jnp.broadcast_to(lax.rsqrt(mean + norm_eps), (64, 128))
        return 0

    lax.fori_loop(0, TOK // 64, square, 0)
    for k in range(8):
        lane = place(k) * FEAT
        gain = t_buf[k, TOK : TOK + 1, :].astype(jnp.float32)

        def norm(i, _):
            at = pl.ds(i * 64, 64)
            v = t_buf[k, at, :].astype(jnp.float32)
            scale = tops[at, :]
            for h in range(2):
                cut = slice(h * 128, h * 128 + 128)
                part = (v[:, cut] * scale * gain[:, cut]).astype(jnp.bfloat16)
                lhs[at, pl.ds(pl.multiple_of(lane + (core ^ h) * 128, 128), 128)] = part
            return 0

        lax.fori_loop(0, TOK // 64, norm, 0)
    tops[...] = jnp.full(tops.shape, -jnp.inf, jnp.float32)
    sums[...] = jnp.zeros(sums.shape, jnp.float32)
    squares[...] = jnp.zeros(squares.shape, jnp.float32)
    picks[...] = jnp.zeros(picks.shape, jnp.float32)
    for c in w_copies:
        c.wait()

    def matmul(step, buf):
        cols = pl.ds(pl.multiple_of(step * COLS, COLS), COLS)
        buf[...] = jnp.dot(lhs[...], w_buf[:, cols], preferred_element_type=jnp.float32)

    lanes = lax.broadcasted_iota(jnp.int32, (32, 128), 1)

    def take(step, buf, masked=False):
        for i in range(TOK // 32):
            at = slice(i * 32, i * 32 + 32)
            old = tops[at, :]
            xs = [buf[at, j * 128 : (j + 1) * 128] for j in range(COLS // 128)]
            ids = ids_ref[at, :] - step * COLS
            new = old
            seen = picks[at, :]
            for j, x in enumerate(xs):
                seen = jnp.where(lanes == ids - j * 128, x, seen)
                if masked:
                    x = xs[j] = jnp.where(lanes < valid - step * COLS - j * 128, x, -jnp.inf)
                new = jnp.maximum(new, x)
            scale = jnp.exp(old - new)
            s = sums[at, :] * scale
            q = squares[at, :] * (scale * scale)
            for x in xs:
                e = jnp.exp(x - new)
                s = s + e
                q = q + e * e
            tops[at, :] = new
            sums[at, :] = s
            squares[at, :] = q
            picks[at, :] = seen

    steps = HALF // COLS
    matmul(0, even)

    def pair(i, _):
        matmul(2 * i + 1, odd)
        take(2 * i, even)
        matmul(2 * i + 2, even)
        take(2 * i + 1, odd)
        return 0

    lax.fori_loop(0, steps // 2 - 1, pair, 0)
    matmul(steps - 1, odd)
    take(steps - 2, even)
    take(steps - 1, odd, masked=True)

    def gather(i):
        at = slice(i * 128, i * 128 + 128)
        lane = lax.broadcasted_iota(jnp.int32, (128, 128), 1)
        per_lane = tops[at, :]
        top = jnp.max(per_lane, axis=1, keepdims=True)
        scale = jnp.exp(per_lane - top)
        s = jnp.sum(sums[at, :] * scale, axis=1, keepdims=True)
        q = jnp.sum(squares[at, :] * (scale * scale), axis=1, keepdims=True)
        p = jnp.sum(picks[at, :], axis=1, keepdims=True)
        tile = jnp.where(lane == 0, top, jnp.where(lane == 1, s, jnp.where(lane == 2, q, p)))
        return jnp.transpose(tile)

    if not last:
        for i in range(TOK // 128):
            rows_t = gather(i)
            for r in range(4):
                out_ref[r * 4 + i : r * 4 + i + 1, :] = rows_t[r : r + 1, :]
        out_ref[16:24, :] = jnp.zeros((8, 128), jnp.float32)
        return
    base = 8 * dp
    away = 8 - base
    for i in range(TOK // 128):
        rows_t = gather(i)
        for r in range(4):
            out_ref[away, r * 4 + i : r * 4 + i + 1, :] = rows_t[r : r + 1, :]
    for j in range(8):
        if j > 0:
            out_ref[away + j, 0:16, :] = out_ref[away, 0:16, :]
        out_ref[away + j, 16:24, :] = jnp.zeros((8, 128), jnp.float32)
        out_ref[base + j, 0:16, :] = first_ref[0:16, :]
        out_ref[base + j, 16:24, :] = ref_ref[...]


def head_stats(where, toks, heads, ids, far_core, first=None, ref=None):
    last = first is not None
    any_spec = pl.BlockSpec(memory_space=pl.ANY)
    vmem = pl.BlockSpec(memory_space=pltpu.VMEM)
    extra = [first, ref] if last else []
    shape = (16, 24, 128) if last else (24, 128)
    flops = 2 * TOK * HALF * 2048
    return pl.pallas_call(
        functools.partial(head_kernel, last, far_core),
        out_shape=jax.ShapeDtypeStruct(shape, jnp.float32),
        in_specs=[pl.BlockSpec(memory_space=pltpu.SMEM)] + [any_spec] * 19 + [vmem] * (1 + len(extra)),
        out_specs=vmem,
        scratch_shapes=[
            pltpu.VMEM((2048, HALF), jnp.bfloat16),
            pltpu.VMEM((8, PART, FEAT), jnp.bfloat16),
            pltpu.VMEM((TOK, 2048), jnp.bfloat16),
            pltpu.VMEM((TOK, 128), jnp.float32),
            pltpu.VMEM((TOK, 128), jnp.float32),
            pltpu.VMEM((TOK, 128), jnp.float32),
            pltpu.VMEM((TOK, 128), jnp.float32),
            pltpu.VMEM((TOK, COLS), jnp.float32),
            pltpu.VMEM((TOK, COLS), jnp.float32),
            pltpu.SemaphoreType.DMA,
            pltpu.SemaphoreType.DMA,
        ],
        compiler_params=pltpu.CompilerParams(vmem_limit_bytes=40 * 1024 * 1024),
        cost_estimate=pl.CostEstimate(flops=flops, bytes_accessed=10 * 2**20, transcendentals=TOK * HALF),
        name="head_last" if last else "head_first",
    )(where, *toks, *heads, ids, *extra)


def combine_kernel(where_ref, got_ref, old_ref, adv_ref, logp_ref, loss_ref, parts_ref):
    dp, length = where_ref[0, 4], where_ref[0, 6]
    tops = got_ref[:, 0:4, :]
    row_max = jnp.max(tops, axis=0)
    scale = jnp.exp(tops - row_max[None])
    exp_sum = jnp.sum(got_ref[:, 4:8, :] * scale, axis=0)
    exp_square = jnp.sum(got_ref[:, 8:12, :] * (scale * scale), axis=0)
    picked = jnp.sum(got_ref[:, 12:16, :], axis=0)
    new_logp = picked - row_max - jnp.log(exp_sum)
    prob_square = exp_square / (exp_sum * exp_sum)

    def rows(ref):
        return jnp.concatenate([ref[:, i * 128 : (i + 1) * 128] for i in range(4)], axis=0)

    ref_rows = [got_ref[8 * dp + i, 16:17, :64] for i in range(8)]
    ref_logp = jnp.concatenate(
        [jnp.concatenate(ref_rows[2 * i : 2 * i + 2], axis=1) for i in range(4)], axis=0
    )
    positions = lax.broadcasted_iota(jnp.int32, (4, 128), 0) * 128
    positions = positions + lax.broadcasted_iota(jnp.int32, (4, 128), 1)
    live_mask = (positions < length).astype(jnp.float32)
    token_loss, kl_part, grad_part = token_terms(
        new_logp, rows(old_ref), rows(adv_ref), ref_logp, live_mask, prob_square
    )
    for i in range(4):
        logp_ref[:, i * 128 : (i + 1) * 128] = new_logp[i : i + 1, :]
        loss_ref[:, i * 128 : (i + 1) * 128] = token_loss[i : i + 1, :]
    lane = lax.broadcasted_iota(jnp.int32, (1, 128), 1)
    line = jnp.zeros((1, 128), jnp.float32)
    for i, term in enumerate((live_mask, token_loss, kl_part, grad_part)):
        total = jnp.sum(jnp.sum(term, axis=0, keepdims=True), axis=1, keepdims=True)
        line = jnp.where(lane == i, total, line)
    parts_ref[...] = jnp.broadcast_to(line[None], (32, 1, 128))


def combine(where, got, old_logp, advantages):
    vmem = pl.BlockSpec(memory_space=pltpu.VMEM)
    line = jax.ShapeDtypeStruct((1, TOK), jnp.float32)
    return pl.pallas_call(
        combine_kernel,
        out_shape=(line, line, jax.ShapeDtypeStruct((32, 1, 128), jnp.float32)),
        in_specs=[pl.BlockSpec(memory_space=pltpu.SMEM)] + [vmem] * 3,
        out_specs=[vmem] * 3,
        name="combine",
    )(where, got, old_logp, advantages)


def token_terms(new_logp, old_logp, advantages, ref_logp, live_mask, prob_square):
    diff = new_logp - old_logp
    prob_ratio = jnp.exp(jnp.clip(diff, -log_limit, log_limit))
    clipped = jnp.clip(prob_ratio, 1.0 - clip_eps, 1.0 + clip_eps)
    plain_term = prob_ratio * advantages
    bounded_term = clipped * advantages
    surrogate = jnp.minimum(plain_term, bounded_term)
    ref_gap = ref_logp - new_logp
    gap_clip = jnp.clip(ref_gap, -log_limit, log_limit)
    kl_term = jnp.exp(gap_clip) - gap_clip - 1.0
    token_loss = live_mask * (kl_coef * kl_term - surrogate)
    inside_gap = (jnp.abs(ref_gap) < log_limit).astype(jnp.float32)
    inside_ratio = (jnp.abs(diff) < log_limit).astype(jnp.float32)
    active_term = (plain_term <= bounded_term).astype(jnp.float32)
    grad_coef = live_mask * (
        kl_coef * (1.0 - jnp.exp(gap_clip)) * inside_gap
        - advantages * prob_ratio * active_term * inside_ratio
    )
    grad_square = grad_coef * grad_coef * (prob_square - 2.0 * jnp.exp(new_logp) + 1.0)
    return (token_loss, live_mask * kl_term, grad_square)


def two_way(n):
    return [(i, (i + 1) % n) for i in range(n)] + [(n + i, n + (i - 1) % n) for i in range(n)]


def one_way(n, core):
    pairs = two_way(n)
    return pairs[n:] if core else pairs[:n]


def passed(block):
    return lax.ppermute(block, "core", shift(2, 1))


def token_ring(own, far_core):
    block = jnp.concatenate([own, passed(own)])
    out = [own]
    for _ in range(3):
        block = lax.ppermute(block, ("core", "tensor"), two_way(8))
        out += [block, passed(block)]
    far = lax.ppermute(block, ("core", "tensor"), one_way(8, far_core))
    return out + [far, passed_from(far, far_core)]


def passed_from(block, core):
    return lax.ppermute(block, "core", [(core, 1 - core)])


def head_ring(own, far_core):
    block = jnp.concatenate([own, passed(own)])
    near = lax.ppermute(block, ("y", "core"), two_way_y())
    far = lax.ppermute(near, ("y", "core"), [p for p in two_way_y() if p[0] % 2 == far_core])
    return [block, near, passed(near), far, passed_from(far, far_core)]


def two_way_y():
    up = [(2 * i, 2 * ((i + 1) % 4)) for i in range(4)]
    down = [(2 * i + 1, 2 * ((i - 1) % 4) + 1) for i in range(4)]
    return up + down


def shards(
    hidden,
    norm_gain,
    head_weight,
    token_ids,
    lengths,
    old_logp,
    advantages,
    rollout_logp,
    rollout_row,
):
    dp, xh, y, core, tensor = [lax.axis_index(a) for a in ("dp", "xh", "y", "core", "tensor")]
    cols = head_weight.shape[1]
    valid = jnp.where(dp == 0, HALF, cols - HALF)
    where = jnp.stack([tensor, xh, y, core, dp, valid, lengths[0], valid]).astype(jnp.int32)[None, :]

    stream = jnp.concatenate([hidden, jnp.broadcast_to(norm_gain[None, :], (16, FEAT))])
    partner = lax.ppermute(stream, "dp", shift(2, 1))
    mine, other = split_head(where, head_weight)
    near = lax.ppermute(other, ("dp", "xh"), X_NEAR)
    own_toks = token_ring(stream, 0)
    heads = head_ring(mine, 0) + head_ring(near, 1)
    partner_toks = token_ring(partner, 1)

    partner_ids = lax.ppermute(token_ids, "dp", shift(2, 1))

    def column_ids(ids):
        local = ids.reshape(-1) - (tensor * cols + dp * HALF)
        local = jnp.where((local >= 0) & (local < valid), local, -1)
        return jnp.broadcast_to(local[:, None], (TOK, 128))

    refs = jnp.broadcast_to(rollout_logp, (32, 1, 64))
    refs = lax.all_to_all(refs, ("dp", "xh", "y", "core"), 0, 0, tiled=True)
    own_ref = lax.dynamic_index_in_dim(refs[:, 0], rollout_row[0], 0)
    own_ref = jnp.pad(own_ref, ((0, 7), (0, 64)))

    first = head_stats(where, own_toks, heads, column_ids(token_ids), 0)
    send = head_stats(where, partner_toks, heads, column_ids(partner_ids), 1, first, own_ref)
    got = lax.all_to_all(send, ("dp", "tensor"), 0, 0, tiled=True)
    new_logp, token_loss, parts = combine(where, got, old_logp, advantages)
    totals = jnp.sum(lax.all_to_all(parts, ("dp", "xh", "y", "core"), 0, 0, tiled=True), axis=(0, 1))
    ratio = totals[1:4] / totals[0]
    summary = jnp.where(lax.iota(jnp.int32, 3) == 2, jnp.sqrt(ratio), ratio)
    return (new_logp, token_loss, summary)


def solution(mesh):
    fine = Mesh(mesh.devices.reshape(2, 2, 4, 2, 8), ("dp", "xh", "y", "core", "tensor"))
    rows = ("dp", "xh", "y", "core")
    in_specs = (
        P(rows, "tensor"),
        P("tensor"),
        P(("xh", "y", "core"), "tensor"),
        P(rows, None),
        P(rows),
        P(rows, None),
        P(rows, None),
        P(rows, "tensor"),
        P(rows),
    )
    out_specs = (P(rows, None), P(rows, None), P())
    return jax.shard_map(shards, mesh=fine, in_specs=in_specs, out_specs=out_specs, check_vma=False)
```

```python
import jax
import jax.numpy as jnp
from jax import lax
from jax.experimental import pallas as pl
from jax.experimental.pallas import tpu as pltpu
from jax.sharding import Mesh, PartitionSpec as P


clip_eps = 0.2
kl_coef = 0.2
log_limit = 10.0
norm_eps = 1e-06

HALF = 2008
ROWS = 128
FEAT = 256
TOK = 512
PART = TOK + 16
TILE = 256


def shift(n, k):
    return [(i, (i + k) % n) for i in range(n)]


def x_position(x):
    return (x % 2) * 2 + x // 2


X_NEAR = [(x_position(a), x_position(b)) for a, b in ((1, 2), (2, 1), (3, 0), (0, 3))]


def prepare_kernel(hidden_ref, gain_ref, ids_ref, head_ref, stream_ref, mine_ref, other_ref, sem):
    dp = lax.axis_index("dp")
    at = pl.multiple_of(dp * HALF, 8)
    away = pl.multiple_of((1 - dp) * HALF, 8)
    copies = [
        pltpu.make_async_copy(head_ref.at[pl.ds(away, HALF)], other_ref, sem),
        pltpu.make_async_copy(head_ref.at[pl.ds(at, HALF)], mine_ref, sem),
    ]
    for c in copies:
        c.start()
    stream_ref[:TOK, :] = hidden_ref[...]
    ids = ids_ref[...]
    digits = [(ids // 256).astype(jnp.float32), (ids % 256).astype(jnp.float32)]
    rows = [gain_ref[...].astype(jnp.float32).reshape(1, FEAT)] + [d[:, h * FEAT : (h + 1) * FEAT] for d in digits for h in range(2)]
    rows.append(jnp.zeros((PART - TOK - 5, FEAT), jnp.float32))
    stream_ref[TOK:, :] = jnp.concatenate(rows, axis=0).astype(jnp.bfloat16)
    for c in copies:
        c.wait()


def prepare(hidden, gain, ids, slices):
    vmem = pl.BlockSpec(memory_space=pltpu.VMEM)
    any_spec = pl.BlockSpec(memory_space=pl.ANY)
    half = jax.ShapeDtypeStruct((HALF, ROWS), jnp.bfloat16)
    return pl.pallas_call(
        prepare_kernel,
        out_shape=(jax.ShapeDtypeStruct((PART, FEAT), jnp.bfloat16), half, half),
        in_specs=[vmem] * 3 + [any_spec],
        out_specs=[vmem] * 3,
        scratch_shapes=[pltpu.SemaphoreType.DMA],
        name="prepare",
    )(hidden, gain, ids, slices)


def head_kernel(*refs):
    tok_sets = [refs[0:8], refs[8:16]]
    heads = refs[16:26]
    ref_ref, out_ref, w_buf, t_buf, *lhs, even, odd, sem_t, sem_p, sem_w = refs[26:]
    dp, xh, y, core, tensor = [lax.axis_index(a) for a in ("dp", "xh", "y", "core", "tensor")]

    def copy(src, dst, sem):
        c = pltpu.make_async_copy(src, dst, sem)
        c.start()
        return c

    sems = (sem_t, sem_p)

    def fetch_tokens(s):
        return [copy(tok_sets[s][k], t_buf.at[s, k], sems[s]) for k in range(8)]

    lanes_of = [pl.ds(i * ROWS, ROWS) for i in range(16)]
    t_copies = [fetch_tokens(0)]
    w_copies = []
    for s in range(2):
        own, near, near_passed, far, far_passed = heads[5 * s : 5 * s + 5]
        at = 8 * s
        for h in range(2):
            w_copies.append(copy(own.at[h], w_buf.at[:, lanes_of[at + h]], sem_w))
            w_copies.append(copy(near.at[h], w_buf.at[:, lanes_of[at + 2 + h]], sem_w))
            w_copies.append(copy(near_passed.at[h], w_buf.at[:, lanes_of[at + 5 - h]], sem_w))
            last = pltpu.make_async_copy(far.at[h], w_buf.at[:, lanes_of[at + 6 + h]], sem_w)
            passed_last = pltpu.make_async_copy(far_passed.at[h], w_buf.at[:, lanes_of[at + 7 - h]], sem_w)

            @pl.when(core == s)
            def _():
                last.start()

            @pl.when(core != s)
            def _():
                passed_last.start()

            w_copies.append(last)
    t_copies.append(fetch_tokens(1))

    way = 2 * core - 1

    def place(k):
        if k == 0:
            offset = 0
        elif k == 7:
            offset = 4
        else:
            step = (k + 1) // 2
            offset = -step if k % 2 == 1 else step
        z = lax.rem(tensor + offset + 8, 8)
        zh, zy = lax.div(z, 4), lax.rem(z, 4)
        step = lax.rem(way * (zy - y) + 4, 4)
        order = jnp.where(step == 0, 0, jnp.where(step == 1, 1, jnp.where(step == 3, 2, 3)))
        return jnp.where(zh == xh, 0, 4) + order

    places = [place(k) * FEAT for k in range(8)]

    def norm(n):
        s, half = divmod(n, 2)
        for i in range(TILE // 32):
            at = slice(half * TILE + i * 32, half * TILE + i * 32 + 32)
            to = slice(i * 32, i * 32 + 32)
            total = None
            for k in range(8):
                v = t_buf[s, k, at, :].astype(jnp.float32)
                v = v * v
                v = v[:, :128] + v[:, 128:]
                total = v if total is None else total + v
            mean = jnp.sum(total, axis=1, keepdims=True) * (1.0 / 2048)
            scale = jnp.broadcast_to(lax.rsqrt(mean + norm_eps), (32, 128))
            for k in range(8):
                v = t_buf[s, k, at, :].astype(jnp.float32)
                gain = t_buf[s, k, TOK : TOK + 1, :].astype(jnp.float32)
                for h in range(2):
                    cut = slice(h * 128, h * 128 + 128)
                    part = (v[:, cut] * scale * gain[:, cut]).astype(jnp.bfloat16)
                    lhs[n][to, pl.ds(pl.multiple_of(places[k] + (core ^ h) * 128, 128), 128)] = part

    for c in t_copies[0]:
        c.wait()
    norm(0)
    for c in t_copies[1]:
        c.wait()
    for c in w_copies:
        c.wait()

    base, away = 8 * dp, 8 - 8 * dp
    start = tensor * (2 * HALF) + dp * HALF

    def matmul(n, buf):
        buf[...] = lax.dot_general(
            w_buf[...],
            lhs[n][...],
            (((1,), (1,)), ((), ())),
            preferred_element_type=jnp.float32,
        )

    cuts = [slice(i, min(i + 64, HALF)) for i in range(0, HALF, 64)]

    def fold(x, op):
        parts = [x[i : i + 8] for i in range(0, x.shape[0], 8)]
        while len(parts) > 1:
            pairs = [op(a, b) for a, b in zip(parts[::2], parts[1::2])]
            parts = pairs + parts[len(parts) // 2 * 2 :]
        return parts[0]

    row = lax.broadcasted_iota(jnp.int32, (64, 128), 0)

    def take(n, buf):
        s, half = divmod(n, 2)
        block = base if s == 0 else away
        for lt in range(TILE // 128):
            lanes = slice(lt * 128, lt * 128 + 128)
            digits = [t_buf[s, 0, TOK + 1 + r : TOK + 2 + r, lanes].astype(jnp.float32) for r in (half, 2 + half)]
            ids = (digits[0] * 256.0 + digits[1]).astype(jnp.int32) - start
            top = None
            for cut in cuts:
                part = fold(buf[cut, lanes], jnp.maximum)
                top = part if top is None else jnp.maximum(top, part)
            top = jnp.max(top, axis=0, keepdims=True)
            total = square = pick = jnp.zeros((8, 128), jnp.float32)
            for cut in cuts:
                x = buf[cut, lanes]
                e = jnp.exp(x - top)
                total = total + fold(e, jnp.add)
                square = square + fold(e * e, jnp.add)
                hit = row[: x.shape[0]] == ids - cut.start
                pick = pick + fold(jnp.where(hit, x, 0.0), jnp.add)
            line = half * 2 + lt
            out_ref[block, line : line + 1, :] = top
            for r, v in ((4, total), (8, square), (12, pick)):
                out_ref[block, r + line : r + line + 1, :] = jnp.sum(v, axis=0, keepdims=True)

    steps = 2 * TOK // TILE
    bufs = (even, odd)
    for n in range(steps):
        matmul(n, bufs[n % 2])
        if n + 1 < steps:
            norm(n + 1)
        if n > 0:
            take(n - 1, bufs[(n - 1) % 2])
    take(steps - 1, bufs[(steps - 1) % 2])
    out_ref[base, 16:24, :] = ref_ref[...]
    out_ref[away, 16:24, :] = ref_ref[...]
    for j in range(1, 8):
        out_ref[base + j] = out_ref[base]
        out_ref[away + j] = out_ref[away]


def head_stats(own_toks, partner_toks, heads, ref):
    any_spec = pl.BlockSpec(memory_space=pl.ANY)
    vmem = pl.BlockSpec(memory_space=pltpu.VMEM)
    return pl.pallas_call(
        head_kernel,
        out_shape=jax.ShapeDtypeStruct((16, 24, 128), jnp.float32),
        in_specs=[any_spec] * 26 + [vmem],
        out_specs=vmem,
        scratch_shapes=[
            pltpu.VMEM((HALF, 2048), jnp.bfloat16),
            pltpu.VMEM((2, 8, PART, FEAT), jnp.bfloat16),
            *[pltpu.VMEM((TILE, 2048), jnp.bfloat16) for _ in range(2 * TOK // TILE)],
            pltpu.VMEM((HALF, TILE), jnp.float32),
            pltpu.VMEM((HALF, TILE), jnp.float32),
            pltpu.SemaphoreType.DMA,
            pltpu.SemaphoreType.DMA,
            pltpu.SemaphoreType.DMA,
        ],
        compiler_params=pltpu.CompilerParams(vmem_limit_bytes=56 * 1024 * 1024),
        cost_estimate=pl.CostEstimate(
            flops=4 * TOK * HALF * 2048, bytes_accessed=13 * 2**20, transcendentals=2 * TOK * HALF
        ),
        name="head_stats",
    )(*own_toks, *partner_toks, *heads, ref)


def combine_kernel(length_ref, got_ref, old_ref, adv_ref, logp_ref, loss_ref, parts_ref):
    dp, length = lax.axis_index("dp"), length_ref[0]
    tops = got_ref[:, 0:4, :]
    row_max = jnp.max(tops, axis=0)
    scale = jnp.exp(tops - row_max[None])
    exp_sum = jnp.sum(got_ref[:, 4:8, :] * scale, axis=0)
    exp_square = jnp.sum(got_ref[:, 8:12, :] * (scale * scale), axis=0)
    picked = jnp.sum(got_ref[:, 12:16, :], axis=0)
    new_logp = picked - row_max - jnp.log(exp_sum)
    prob_square = exp_square / (exp_sum * exp_sum)

    def rows(ref):
        return jnp.concatenate([ref[:, i * 128 : (i + 1) * 128] for i in range(4)], axis=0)

    ref_rows = [got_ref[8 * dp + i, 16:17, :64] for i in range(8)]
    ref_logp = jnp.concatenate(
        [jnp.concatenate(ref_rows[2 * i : 2 * i + 2], axis=1) for i in range(4)], axis=0
    )
    positions = lax.broadcasted_iota(jnp.int32, (4, 128), 0) * 128
    positions = positions + lax.broadcasted_iota(jnp.int32, (4, 128), 1)
    live_mask = (positions < length).astype(jnp.float32)
    token_loss, kl_part, grad_part = token_terms(
        new_logp, rows(old_ref), rows(adv_ref), ref_logp, live_mask, prob_square
    )
    for i in range(4):
        logp_ref[:, i * 128 : (i + 1) * 128] = new_logp[i : i + 1, :]
        loss_ref[:, i * 128 : (i + 1) * 128] = token_loss[i : i + 1, :]
    lane = lax.broadcasted_iota(jnp.int32, (1, 128), 1)
    line = jnp.zeros((1, 128), jnp.float32)
    for i, term in enumerate((live_mask, token_loss, kl_part, grad_part)):
        total = jnp.sum(jnp.sum(term, axis=0, keepdims=True), axis=1, keepdims=True)
        line = jnp.where(lane == i, total, line)
    parts_ref[...] = jnp.broadcast_to(line[None], (32, 1, 128))


def combine(lengths, got, old_logp, advantages):
    vmem = pl.BlockSpec(memory_space=pltpu.VMEM)
    line = jax.ShapeDtypeStruct((1, TOK), jnp.float32)
    return pl.pallas_call(
        combine_kernel,
        out_shape=(line, line, jax.ShapeDtypeStruct((32, 1, 128), jnp.float32)),
        in_specs=[pl.BlockSpec(memory_space=pltpu.SMEM)] + [vmem] * 3,
        out_specs=[vmem] * 3,
        name="combine",
    )(lengths, got, old_logp, advantages)


def token_terms(new_logp, old_logp, advantages, ref_logp, live_mask, prob_square):
    diff = new_logp - old_logp
    prob_ratio = jnp.exp(jnp.clip(diff, -log_limit, log_limit))
    clipped = jnp.clip(prob_ratio, 1.0 - clip_eps, 1.0 + clip_eps)
    plain_term = prob_ratio * advantages
    bounded_term = clipped * advantages
    surrogate = jnp.minimum(plain_term, bounded_term)
    ref_gap = ref_logp - new_logp
    gap_clip = jnp.clip(ref_gap, -log_limit, log_limit)
    kl_term = jnp.exp(gap_clip) - gap_clip - 1.0
    token_loss = live_mask * (kl_coef * kl_term - surrogate)
    inside_gap = (jnp.abs(ref_gap) < log_limit).astype(jnp.float32)
    inside_ratio = (jnp.abs(diff) < log_limit).astype(jnp.float32)
    active_term = (plain_term <= bounded_term).astype(jnp.float32)
    grad_coef = live_mask * (
        kl_coef * (1.0 - jnp.exp(gap_clip)) * inside_gap
        - advantages * prob_ratio * active_term * inside_ratio
    )
    grad_square = grad_coef * grad_coef * (prob_square - 2.0 * jnp.exp(new_logp) + 1.0)
    return (token_loss, live_mask * kl_term, grad_square)


def two_way_y():
    up = [(2 * i, 2 * ((i + 1) % 4)) for i in range(4)]
    down = [(2 * i + 1, 2 * ((i - 1) % 4) + 1) for i in range(4)]
    return up + down


def token_ring(own, far_step):
    back, ahead = own, own
    out = [own]
    for _ in range(1, 4):
        back = lax.ppermute(back, "tensor", shift(8, 1))
        ahead = lax.ppermute(ahead, "tensor", shift(8, -1))
        out += [back, ahead]
    far = back if far_step > 0 else ahead
    return out + [lax.ppermute(far, "tensor", shift(8, far_step))]


def head_ring(block, far_core):
    near = lax.ppermute(block, ("y", "core"), two_way_y())
    pairs = [p for p in two_way_y() if p[0] % 2 == far_core]
    far = lax.ppermute(near, ("y", "core"), pairs)
    near_passed = lax.ppermute(near, "core", shift(2, 1))
    far_passed = lax.ppermute(far, "core", [(far_core, 1 - far_core)])
    return [block, near, near_passed, far, far_passed]


def steps(hidden, norm_gain, head_weight, token_ids, lengths, old_logp, advantages, rollout_logp, rollout_row):
    slices = head_weight.T
    stream, mine, other = prepare(hidden, norm_gain, token_ids, slices)
    partner = lax.ppermute(stream, "dp", shift(2, 1))
    own_toks = token_ring(stream, 1)

    near = lax.ppermute(other, ("dp", "xh"), X_NEAR)
    heads = head_ring(jnp.stack([mine, lax.ppermute(mine, "core", shift(2, 1))]), 0)
    heads += head_ring(jnp.stack([near, lax.ppermute(near, "core", shift(2, 1))]), 1)
    partner_toks = token_ring(partner, -1)

    refs = jnp.broadcast_to(rollout_logp, (32, 1, 64))
    refs = lax.all_to_all(refs, ("dp", "xh", "y", "core"), 0, 0, tiled=True)
    own_ref = lax.dynamic_index_in_dim(refs[:, 0], rollout_row[0], 0)
    own_ref = jnp.pad(own_ref, ((0, 7), (0, 64)))

    send = head_stats(own_toks, partner_toks, heads, own_ref)
    got = lax.all_to_all(send, ("dp", "tensor"), 0, 0, tiled=True)
    new_logp, token_loss, parts = combine(lengths, got, old_logp, advantages)
    totals = jnp.sum(lax.all_to_all(parts, ("dp", "xh", "y", "core"), 0, 0, tiled=True), axis=(0, 1))
    ratio = totals[1:4] / totals[0]
    summary = jnp.where(lax.iota(jnp.int32, 3) == 2, jnp.sqrt(ratio), ratio)
    return (new_logp, token_loss, summary)


def solution(mesh):
    fine = Mesh(mesh.devices.reshape(2, 2, 4, 2, 8), ("dp", "xh", "y", "core", "tensor"))
    rows = ("dp", "xh", "y", "core")
    in_specs = (
        P(rows, "tensor"),
        P("tensor"),
        P(("xh", "y", "core"), "tensor"),
        P(rows, None),
        P(rows),
        P(rows, None),
        P(rows, None),
        P(rows, "tensor"),
        P(rows),
    )
    out_specs = (P(rows, None), P(rows, None), P())
    return jax.shard_map(steps, mesh=fine, in_specs=in_specs, out_specs=out_specs, check_vma=False)
```

```python
import jax
import jax.numpy as jnp
from jax import lax
from jax.experimental import pallas as pl
from jax.experimental.pallas import tpu as pltpu
from jax.sharding import Mesh, PartitionSpec as P


clip_eps = 0.2
kl_coef = 0.2
log_limit = 10.0
norm_eps = 1e-06

HALF = 2008
ROWS = 128
FEAT = 256
TOK = 512
PART = TOK + 16
TILE = 256


def shift(n, k):
    return [(i, (i + k) % n) for i in range(n)]


def x_position(x):
    return (x % 2) * 2 + x // 2


X_NEAR = [(x_position(a), x_position(b)) for a, b in ((1, 2), (2, 1), (3, 0), (0, 3))]


def prepare_kernel(
    hidden_ref, gain_ref, ids_ref, logp_ref, head_ref, stream_ref, mine_ref, other_ref, rows_ref, sem
):
    dp = lax.axis_index("dp")
    at = pl.multiple_of(dp * HALF, 8)
    away = pl.multiple_of((1 - dp) * HALF, 8)
    copies = [
        pltpu.make_async_copy(head_ref.at[pl.ds(away, HALF)], other_ref, sem),
        pltpu.make_async_copy(head_ref.at[pl.ds(at, HALF)], mine_ref, sem),
    ]
    for c in copies:
        c.start()
    rows_ref[...] = jnp.broadcast_to(logp_ref[...][None], rows_ref.shape)
    stream_ref[:TOK, :] = hidden_ref[...]
    ids = ids_ref[...]
    digits = [(ids // 256).astype(jnp.float32), (ids % 256).astype(jnp.float32)]
    rows = [gain_ref[...].astype(jnp.float32).reshape(1, FEAT)] + [d[:, h * FEAT : (h + 1) * FEAT] for d in digits for h in range(2)]
    rows.append(jnp.zeros((PART - TOK - 5, FEAT), jnp.float32))
    stream_ref[TOK:, :] = jnp.concatenate(rows, axis=0).astype(jnp.bfloat16)
    for c in copies:
        c.wait()


def prepare(hidden, gain, ids, logp, slices):
    vmem = pl.BlockSpec(memory_space=pltpu.VMEM)
    any_spec = pl.BlockSpec(memory_space=pl.ANY)
    half = jax.ShapeDtypeStruct((HALF, ROWS), jnp.bfloat16)
    return pl.pallas_call(
        prepare_kernel,
        out_shape=(
            jax.ShapeDtypeStruct((PART, FEAT), jnp.bfloat16),
            half,
            half,
            jax.ShapeDtypeStruct((32, 1, 64), jnp.float32),
        ),
        in_specs=[vmem] * 4 + [any_spec],
        out_specs=[vmem] * 4,
        scratch_shapes=[pltpu.SemaphoreType.DMA],
        name="prepare",
    )(hidden, gain, ids, logp, slices)


def head_kernel(*refs):
    tok_sets = [refs[0:8], refs[8:16]]
    heads = refs[16:26]
    ref_ref, out_ref, w_buf, t_buf, *lhs, even, odd, sem_t, sem_p, sem_w = refs[26:]
    dp, xh, y, core, tensor = [lax.axis_index(a) for a in ("dp", "xh", "y", "core", "tensor")]

    def copy(src, dst, sem):
        c = pltpu.make_async_copy(src, dst, sem)
        c.start()
        return c

    sems = (sem_t, sem_p)

    def fetch_tokens(s):
        return [copy(tok_sets[s][k], t_buf.at[s, k], sems[s]) for k in range(8)]

    lanes_of = [pl.ds(i * ROWS, ROWS) for i in range(16)]
    t_copies = [fetch_tokens(0)]
    w_copies = []
    for s in range(2):
        own, near, near_passed, far, far_passed = heads[5 * s : 5 * s + 5]
        at = 8 * s
        for h in range(2):
            w_copies.append(copy(own.at[h], w_buf.at[:, lanes_of[at + h]], sem_w))
            w_copies.append(copy(near.at[h], w_buf.at[:, lanes_of[at + 2 + h]], sem_w))
            w_copies.append(copy(near_passed.at[h], w_buf.at[:, lanes_of[at + 5 - h]], sem_w))
            last = pltpu.make_async_copy(far.at[h], w_buf.at[:, lanes_of[at + 6 + h]], sem_w)
            passed_last = pltpu.make_async_copy(far_passed.at[h], w_buf.at[:, lanes_of[at + 7 - h]], sem_w)

            @pl.when(core == s)
            def _():
                last.start()

            @pl.when(core != s)
            def _():
                passed_last.start()

            w_copies.append(last)
    t_copies.append(fetch_tokens(1))

    way = 2 * core - 1

    def place(k):
        if k == 0:
            offset = 0
        elif k == 7:
            offset = 4
        else:
            step = (k + 1) // 2
            offset = -step if k % 2 == 1 else step
        z = lax.rem(tensor + offset + 8, 8)
        zh, zy = lax.div(z, 4), lax.rem(z, 4)
        step = lax.rem(way * (zy - y) + 4, 4)
        order = jnp.where(step == 0, 0, jnp.where(step == 1, 1, jnp.where(step == 3, 2, 3)))
        return jnp.where(zh == xh, 0, 4) + order

    places = [place(k) * FEAT for k in range(8)]

    def norm(n):
        s, half = divmod(n, 2)
        for i in range(TILE // 32):
            at = slice(half * TILE + i * 32, half * TILE + i * 32 + 32)
            to = slice(i * 32, i * 32 + 32)
            total = None
            for k in range(8):
                v = t_buf[s, k, at, :].astype(jnp.float32)
                v = v * v
                v = v[:, :128] + v[:, 128:]
                total = v if total is None else total + v
            mean = jnp.sum(total, axis=1, keepdims=True) * (1.0 / 2048)
            scale = jnp.broadcast_to(lax.rsqrt(mean + norm_eps), (32, 128))
            for k in range(8):
                v = t_buf[s, k, at, :].astype(jnp.float32)
                gain = t_buf[s, k, TOK : TOK + 1, :].astype(jnp.float32)
                for h in range(2):
                    cut = slice(h * 128, h * 128 + 128)
                    part = (v[:, cut] * scale * gain[:, cut]).astype(jnp.bfloat16)
                    lhs[n][to, pl.ds(pl.multiple_of(places[k] + (core ^ h) * 128, 128), 128)] = part

    for c in t_copies[0]:
        c.wait()
    norm(0)
    for c in t_copies[1]:
        c.wait()
    for c in w_copies:
        c.wait()

    base, away = 8 * dp, 8 - 8 * dp
    start = tensor * (2 * HALF) + dp * HALF

    def matmul(n, buf):
        buf[...] = lax.dot_general(
            w_buf[...],
            lhs[n][...],
            (((1,), (1,)), ((), ())),
            preferred_element_type=jnp.float32,
        )

    cuts = [slice(i, min(i + 64, HALF)) for i in range(0, HALF, 64)]

    def fold(x, op):
        parts = [x[i : i + 8] for i in range(0, x.shape[0], 8)]
        while len(parts) > 1:
            pairs = [op(a, b) for a, b in zip(parts[::2], parts[1::2])]
            parts = pairs + parts[len(parts) // 2 * 2 :]
        return parts[0]

    row = lax.broadcasted_iota(jnp.int32, (64, 128), 0)

    def take(n, buf):
        s, half = divmod(n, 2)
        block = base if s == 0 else away
        for lt in range(TILE // 128):
            lanes = slice(lt * 128, lt * 128 + 128)
            digits = [t_buf[s, 0, TOK + 1 + r : TOK + 2 + r, lanes].astype(jnp.float32) for r in (half, 2 + half)]
            ids = (digits[0] * 256.0 + digits[1]).astype(jnp.int32) - start
            top = None
            for cut in cuts:
                part = fold(buf[cut, lanes], jnp.maximum)
                top = part if top is None else jnp.maximum(top, part)
            top = jnp.max(top, axis=0, keepdims=True)
            total = square = pick = jnp.zeros((8, 128), jnp.float32)
            for cut in cuts:
                x = buf[cut, lanes]
                e = jnp.exp(x - top)
                total = total + fold(e, jnp.add)
                square = square + fold(e * e, jnp.add)
                hit = row[: x.shape[0]] == ids - cut.start
                pick = pick + fold(jnp.where(hit, x, 0.0), jnp.add)
            line = half * 2 + lt
            out_ref[block, line : line + 1, :] = top
            for r, v in ((4, total), (8, square), (12, pick)):
                out_ref[block, r + line : r + line + 1, :] = jnp.sum(v, axis=0, keepdims=True)

    steps = 2 * TOK // TILE
    bufs = (even, odd)
    for n in range(steps):
        matmul(n, bufs[n % 2])
        if n + 1 < steps:
            norm(n + 1)
        if n > 0:
            take(n - 1, bufs[(n - 1) % 2])
    take(steps - 1, bufs[(steps - 1) % 2])
    for block in (base, away):
        out_ref[block, 16:24, :] = jnp.zeros((8, 128), jnp.float32)
        out_ref[block, 16:17, :64] = ref_ref[...]
    for j in range(1, 8):
        out_ref[base + j] = out_ref[base]
        out_ref[away + j] = out_ref[away]


def head_stats(own_toks, partner_toks, heads, ref):
    any_spec = pl.BlockSpec(memory_space=pl.ANY)
    vmem = pl.BlockSpec(memory_space=pltpu.VMEM)
    return pl.pallas_call(
        head_kernel,
        out_shape=jax.ShapeDtypeStruct((16, 24, 128), jnp.float32),
        in_specs=[any_spec] * 26 + [vmem],
        out_specs=vmem,
        scratch_shapes=[
            pltpu.VMEM((HALF, 2048), jnp.bfloat16),
            pltpu.VMEM((2, 8, PART, FEAT), jnp.bfloat16),
            *[pltpu.VMEM((TILE, 2048), jnp.bfloat16) for _ in range(2 * TOK // TILE)],
            pltpu.VMEM((HALF, TILE), jnp.float32),
            pltpu.VMEM((HALF, TILE), jnp.float32),
            pltpu.SemaphoreType.DMA,
            pltpu.SemaphoreType.DMA,
            pltpu.SemaphoreType.DMA,
        ],
        compiler_params=pltpu.CompilerParams(vmem_limit_bytes=56 * 1024 * 1024),
        cost_estimate=pl.CostEstimate(
            flops=4 * TOK * HALF * 2048, bytes_accessed=13 * 2**20, transcendentals=2 * TOK * HALF
        ),
        name="head_stats",
    )(*own_toks, *partner_toks, *heads, ref)


def combine_kernel(length_ref, got_ref, old_ref, adv_ref, logp_ref, loss_ref, parts_ref):
    dp, length = lax.axis_index("dp"), length_ref[0]
    tops = got_ref[:, 0:4, :]
    row_max = jnp.max(tops, axis=0)
    scale = jnp.exp(tops - row_max[None])
    exp_sum = jnp.sum(got_ref[:, 4:8, :] * scale, axis=0)
    exp_square = jnp.sum(got_ref[:, 8:12, :] * (scale * scale), axis=0)
    picked = jnp.sum(got_ref[:, 12:16, :], axis=0)
    new_logp = picked - row_max - jnp.log(exp_sum)
    prob_square = exp_square / (exp_sum * exp_sum)

    def rows(ref):
        return jnp.concatenate([ref[:, i * 128 : (i + 1) * 128] for i in range(4)], axis=0)

    ref_rows = [got_ref[8 * dp + i, 16:17, :64] for i in range(8)]
    ref_logp = jnp.concatenate(
        [jnp.concatenate(ref_rows[2 * i : 2 * i + 2], axis=1) for i in range(4)], axis=0
    )
    positions = lax.broadcasted_iota(jnp.int32, (4, 128), 0) * 128
    positions = positions + lax.broadcasted_iota(jnp.int32, (4, 128), 1)
    live_mask = (positions < length).astype(jnp.float32)
    token_loss, kl_part, grad_part = token_terms(
        new_logp, rows(old_ref), rows(adv_ref), ref_logp, live_mask, prob_square
    )
    for i in range(4):
        logp_ref[:, i * 128 : (i + 1) * 128] = new_logp[i : i + 1, :]
        loss_ref[:, i * 128 : (i + 1) * 128] = token_loss[i : i + 1, :]
    lane = lax.broadcasted_iota(jnp.int32, (1, 128), 1)
    line = jnp.zeros((1, 128), jnp.float32)
    for i, term in enumerate((live_mask, token_loss, kl_part, grad_part)):
        total = jnp.sum(jnp.sum(term, axis=0, keepdims=True), axis=1, keepdims=True)
        line = jnp.where(lane == i, total, line)
    parts_ref[...] = jnp.broadcast_to(line[None], (32, 1, 128))


def combine(lengths, got, old_logp, advantages):
    vmem = pl.BlockSpec(memory_space=pltpu.VMEM)
    line = jax.ShapeDtypeStruct((1, TOK), jnp.float32)
    return pl.pallas_call(
        combine_kernel,
        out_shape=(line, line, jax.ShapeDtypeStruct((32, 1, 128), jnp.float32)),
        in_specs=[pl.BlockSpec(memory_space=pltpu.SMEM)] + [vmem] * 3,
        out_specs=[vmem] * 3,
        name="combine",
    )(lengths, got, old_logp, advantages)


def token_terms(new_logp, old_logp, advantages, ref_logp, live_mask, prob_square):
    diff = new_logp - old_logp
    prob_ratio = jnp.exp(jnp.clip(diff, -log_limit, log_limit))
    clipped = jnp.clip(prob_ratio, 1.0 - clip_eps, 1.0 + clip_eps)
    plain_term = prob_ratio * advantages
    bounded_term = clipped * advantages
    surrogate = jnp.minimum(plain_term, bounded_term)
    ref_gap = ref_logp - new_logp
    gap_clip = jnp.clip(ref_gap, -log_limit, log_limit)
    kl_term = jnp.exp(gap_clip) - gap_clip - 1.0
    token_loss = live_mask * (kl_coef * kl_term - surrogate)
    inside_gap = (jnp.abs(ref_gap) < log_limit).astype(jnp.float32)
    inside_ratio = (jnp.abs(diff) < log_limit).astype(jnp.float32)
    active_term = (plain_term <= bounded_term).astype(jnp.float32)
    grad_coef = live_mask * (
        kl_coef * (1.0 - jnp.exp(gap_clip)) * inside_gap
        - advantages * prob_ratio * active_term * inside_ratio
    )
    grad_square = grad_coef * grad_coef * (prob_square - 2.0 * jnp.exp(new_logp) + 1.0)
    return (token_loss, live_mask * kl_term, grad_square)


def two_way_y():
    up = [(2 * i, 2 * ((i + 1) % 4)) for i in range(4)]
    down = [(2 * i + 1, 2 * ((i - 1) % 4) + 1) for i in range(4)]
    return up + down


def token_ring(own, far_step):
    back, ahead = own, own
    out = [own]
    for _ in range(1, 4):
        back = lax.ppermute(back, "tensor", shift(8, 1))
        ahead = lax.ppermute(ahead, "tensor", shift(8, -1))
        out += [back, ahead]
    far = back if far_step > 0 else ahead
    return out + [lax.ppermute(far, "tensor", shift(8, far_step))]


def head_ring(block, far_core):
    near = lax.ppermute(block, ("y", "core"), two_way_y())
    pairs = [p for p in two_way_y() if p[0] % 2 == far_core]
    far = lax.ppermute(near, ("y", "core"), pairs)
    near_passed = lax.ppermute(near, "core", shift(2, 1))
    far_passed = lax.ppermute(far, "core", [(far_core, 1 - far_core)])
    return [block, near, near_passed, far, far_passed]


def steps(hidden, norm_gain, head_weight, token_ids, lengths, old_logp, advantages, rollout_logp, rollout_row):
    slices = head_weight.T
    stream, mine, other, rows = prepare(hidden, norm_gain, token_ids, rollout_logp, slices)
    partner = lax.ppermute(stream, "dp", shift(2, 1))
    own_toks = token_ring(stream, 1)

    near = lax.ppermute(other, ("dp", "xh"), X_NEAR)
    heads = head_ring(jnp.stack([mine, lax.ppermute(mine, "core", shift(2, 1))]), 0)
    heads += head_ring(jnp.stack([near, lax.ppermute(near, "core", shift(2, 1))]), 1)
    partner_toks = token_ring(partner, -1)

    refs = lax.all_to_all(rows, ("dp", "xh", "y", "core"), 0, 0, tiled=True)
    own_ref = lax.dynamic_index_in_dim(refs[:, 0], rollout_row[0], 0)

    send = head_stats(own_toks, partner_toks, heads, own_ref)
    got = lax.all_to_all(send, ("dp", "tensor"), 0, 0, tiled=True)
    new_logp, token_loss, parts = combine(lengths, got, old_logp, advantages)
    totals = jnp.sum(lax.all_to_all(parts, ("dp", "xh", "y", "core"), 0, 0, tiled=True), axis=(0, 1))
    ratio = totals[1:4] / totals[0]
    summary = jnp.where(lax.iota(jnp.int32, 3) == 2, jnp.sqrt(ratio), ratio)
    return (new_logp, token_loss, summary)


def solution(mesh):
    fine = Mesh(mesh.devices.reshape(2, 2, 4, 2, 8), ("dp", "xh", "y", "core", "tensor"))
    rows = ("dp", "xh", "y", "core")
    in_specs = (
        P(rows, "tensor"),
        P("tensor"),
        P(("xh", "y", "core"), "tensor"),
        P(rows, None),
        P(rows),
        P(rows, None),
        P(rows, None),
        P(rows, "tensor"),
        P(rows),
    )
    out_specs = (P(rows, None), P(rows, None), P())
    return jax.shard_map(steps, mesh=fine, in_specs=in_specs, out_specs=out_specs, check_vma=False)
```
